256 devices in a mesh: dp: 64 (over z, x, core), tensor: 4 (over y).
Axes of the slice: x: 4, y: 4, z: 8, core: 2. Of those that a mesh axis runs over, the one named last changes fastest.
Arguments:
- master_old: float32 [3072, 36864], P('dp', 'tensor'), may hold values from -6 to 6
- moment1_old: float32 [3072, 36864], P('dp', 'tensor'), may hold values from -4 to 4
- moment2_old: float32 [3072, 36864], P('dp', 'tensor'), may hold values from 0.0001 to 1
- grad: bfloat16 [3072, 36864], P('dp', 'tensor'), may hold values from -28 to 28
- send_slots: int32 [64, 1728], P('dp'), may hold values from 0 to 1727, each once within a row
- recv_slots: int32 [64, 1728], P('dp'), may hold values from 0 to 1727, each once within a row
Outputs:
- master_new: float32 [3072, 36864], P('dp', 'tensor')
- moment1_new: float32 [3072, 36864], P('dp', 'tensor')
- moment2_new: float32 [3072, 36864], P('dp', 'tensor')
The draws below stay inside these ranges and needn't reach their ends.
Inputs may be any that keep to these rules, and one draw needn't show every extreme that they name: `send_slots`: each row is a permutation of 0 to 1727; entry [i, j * 27 + q] is the old slot of the q-th block that device i of dp sends to device j. `recv_slots`: each row is a permutation of 0 to 1727; entry [j, i * 27 + q] is the new slot on device j of the q-th block from device i.
All inputs are finite; a program needn't handle non-finite values.
Results may differ from the reference program's by a relative error of at most 0.0003.
Values sent between devices are 32-bit elements; how exact they have to be, the bound alone decides.
No kernel may reach another device: no remote copies, remote signals or barrier semaphores. Data moves between devices by JAX's collectives and lax.ppermute only.
A program may use at most 64 MiB of HBM per device.

```python
import math
import jax
import jax.numpy as jnp

ROWS = 3072
FF = 36864
SEGW = 128
RD = 48
COLS = 9216
HALF = 4608
NSEG = 36
BLK_DEV = 1728
PER_PEER = 27
N_DP = 64
N_TENSOR = 4


def draw_grad(key, part):
    base_key = jax.random.fold_in(key, 11)
    key_base, key_column = jax.random.split(base_key, 2)
    position = jnp.arange(ROWS, dtype=jnp.float32) / (ROWS - 1)
    column_log = jax.random.uniform(key_column, (FF,), jnp.float32, -1.15, 1.15)
    column_scale = jnp.exp(column_log) / 1.465
    row_scale = jnp.power(10.0, position - 0.5) / 1.4664
    values = jax.random.truncated_normal(key_base, -6.0, 6.0, (ROWS, FF), jnp.float32)
    return (values * row_scale[:, None] * column_scale[None, :]).astype(jnp.bfloat16)


def steps_of(stream_key, shape, cuts, low, largest):
    factor_of = 1.0
    for axis_at, blocks in cuts:
        draws = jax.random.uniform(jax.random.fold_in(jax.random.fold_in(stream_key, 6), axis_at), (blocks,), jnp.float32, low / len(cuts), largest / len(cuts))
        factor_of = factor_of * jnp.repeat(jnp.exp(draws), shape[axis_at] // blocks).reshape((-1,) + (1,) * (len(shape) - 1 - axis_at))
    return factor_of


def bell_draw(rng, dims, width, most, shards=(), kind=jnp.bfloat16):
    array = width * jax.random.normal(rng, dims, jnp.float32)
    if shards:
        array = array * steps_of(rng, dims, shards, -0.22, 0.18)
    return jnp.clip(array, -most, most).astype(kind)


def setup_inputs(seed: int = 0) -> dict:
    streams_of = jax.random.split(jax.random.key(seed), 7)
    return {
        "master_old": bell_draw(streams_of[0], (ROWS, FF), 1.0, 6.0, ((0, 64), (1, 4)), jnp.float32),
        "moment1_old": bell_draw(streams_of[1], (ROWS, FF), 0.3, 4.0, ((0, 64), (1, 4)), jnp.float32),
        "moment2_old": jnp.clip(jnp.exp(math.log(1.0) - 9.2103404 * jax.random.uniform(streams_of[2], (ROWS, FF), jnp.float32) ** steps_of(streams_of[2], (ROWS, FF), ((0, 64), (1, 4)), -0.2, 0.2)), 0.0001, 1.0),
        "grad": draw_grad(jax.random.fold_in(streams_of[6], 71), 0),
        "send_slots": jax.vmap(lambda own: jax.random.permutation(own, BLK_DEV))(jax.random.split(streams_of[4], N_DP)).reshape((N_DP, BLK_DEV)).astype(jnp.int32),
        "recv_slots": jax.vmap(lambda own: jax.random.permutation(own, BLK_DEV))(jax.random.split(streams_of[5], N_DP)).reshape((N_DP, BLK_DEV)).astype(jnp.int32),
    }


beta_one = 0.9
beta_two = 0.95
correct_one = 0.6513215599
correct_two = 0.4012630608
adam_eps = 1e-08
learning_rate = 0.01
weight_decay = 0.1
clip_ratio = 0.75

def move_shard(shard, send_slots, recv_slots):
    tiles = shard.reshape(N_DP, RD, 2, NSEG, SEGW).transpose(0, 1, 3, 2, 4).reshape(N_DP, BLK_DEV, 2, SEGW)
    outgoing = jnp.take_along_axis(tiles, send_slots[:, :, None, None], axis=1)
    arrived = outgoing.reshape(N_DP, N_DP, PER_PEER, 2, SEGW).transpose(1, 0, 2, 3, 4).reshape(N_DP, BLK_DEV, 2, SEGW)
    sources = jnp.arange(N_DP, dtype=jnp.int32)[:, None]
    placed = jnp.zeros_like(arrived).at[sources, recv_slots].set(arrived)
    return placed.reshape(N_DP, RD, NSEG, 2, SEGW).transpose(0, 1, 3, 2, 4).reshape(ROWS, COLS)

def reshard(matrix, send_slots, recv_slots):
    moved = [move_shard(matrix[:, shard_index * COLS:(shard_index + 1) * COLS], send_slots, recv_slots) for shard_index in range(N_TENSOR)]
    pieces = []
    for pair_index in range(N_TENSOR // 2):
        first = moved[2 * pair_index]
        second = moved[2 * pair_index + 1]
        pieces.append(first[:, :HALF])
        pieces.append(second[:, :HALF])
        pieces.append(first[:, HALF:])
        pieces.append(second[:, HALF:])
    return jnp.concatenate(pieces, axis=1)

def reference(master_old, moment1_old, moment2_old, grad, send_slots, recv_slots):
    new_master = reshard(master_old, send_slots, recv_slots)
    new_first = reshard(moment1_old, send_slots, recv_slots)
    new_second = reshard(moment2_old, send_slots, recv_slots)
    wide = grad.astype(jnp.float32)
    sum_squares = jnp.sum(wide * wide)
    limit = clip_ratio * jnp.sqrt(jnp.float32(ROWS * FF))
    clip_scale = jnp.minimum(1.0, limit / jnp.sqrt(sum_squares + 1e-06))
    scaled = clip_scale * wide
    moment1 = beta_one * new_first + (1.0 - beta_one) * scaled
    moment2 = beta_two * new_second + (1.0 - beta_two) * scaled * scaled
    update = moment1 / correct_one / (jnp.sqrt(moment2 / correct_two) + adam_eps)
    master = new_master - learning_rate * (update + weight_decay * new_master)
    return (master, moment1, moment2)
```

```python
import jax
import jax.numpy as jnp
from jax import lax
from jax.experimental import pallas as pl
from jax.experimental.pallas import tpu as pltpu
from jax.sharding import Mesh
from jax.sharding import PartitionSpec as P

SEGW = 128
SUB = 8
DP = ("dp_0", "dp_1", "dp_2")
DP_TENSOR = ("dp_0", "dp_1", "dp_2", "pair", "side")
DP_SIDE = ("dp_0", "dp_1", "dp_2", "side")
PAD = 8

beta_one = 0.9
beta_two = 0.95
correct_one = 0.6513215599
correct_two = 0.4012630608
adam_eps = 1e-08
learning_rate = 0.01
weight_decay = 0.1
clip_ratio = 0.75


def tiled(x, groups, half_rows):
    rows, columns = x.shape
    tiles = x.reshape(groups, SUB, columns // SEGW, SEGW).transpose(0, 2, 1, 3)
    return tiles.reshape(groups, 2, half_rows, SEGW)


def untiled(x, rows, columns):
    groups = rows // SUB
    tiles = x.reshape(groups, columns // SEGW, SUB, SEGW).transpose(0, 2, 1, 3)
    return tiles.reshape(rows, columns)


def in_hbm(x):
    return pltpu.with_memory_space_constraint(x, pltpu.HBM)


def slot_rows(slots, segments, span):
    r = lax.shift_right_logical(slots * (-(-65536 // segments)), 16)
    s = slots - r * segments
    return lax.shift_right_logical(r, 3) * (6 * span) + s * SUB + (r & (SUB - 1))


def pack(xs, slots, devices, per_peer, segments):
    groups, _, half_rows, _ = xs[0].shape
    span = half_rows + PAD
    blocks = devices * per_peer
    message = 3 * per_peer
    at_once = 8
    part = at_once * 2 * message

    def kernel(x0, x1, x2, slot_ref, out, mark, held, sent, slot_v, row_v, row_s, sems, out_sems, row_sems):
        to_vmem = pltpu.make_async_copy(slot_ref, slot_v, row_sems.at[0])
        to_vmem.start()
        copies = []
        for g in range(groups):
            for k in range(2):
                for a, x in enumerate((x0, x1, x2)):
                    at = 6 * g + 3 * k + a
                    copies.append(
                        pltpu.make_async_copy(
                            x.at[g, k], held.at[pl.ds(at * span, half_rows)], sems.at[at]
                        )
                    )
        for c in copies:
            c.start()
        to_vmem.wait()
        row_v[...] = slot_rows(slot_v[...], segments, span)
        to_smem = pltpu.make_async_copy(row_v, row_s, row_sems.at[1])
        to_smem.start()
        mark[...] = jnp.zeros_like(mark)
        to_smem.wait()
        for c in copies:
            c.wait()

        def peer(j, carry):
            for q in range(per_peer):
                row = row_s[0, j * per_peer + q]
                sent[pl.ds(j * 2 * message + q, 6, stride=per_peer), :] = held[
                    pl.ds(row, 6, stride=span), :
                ]
            return carry

        leaving = []
        for n in range(devices // at_once):
            lax.fori_loop(n * at_once, (n + 1) * at_once, peer, 0)
            rows = pl.ds(n * part, part)
            leaving.append(pltpu.make_async_copy(sent.at[rows], out.at[rows], out_sems.at[n]))
            leaving[-1].start()
        for c in leaving:
            c.wait()

    hbm = pl.BlockSpec(memory_space=pltpu.HBM)
    vmem = pl.BlockSpec(memory_space=pltpu.VMEM)
    return pl.pallas_call(
        kernel,
        out_shape=(
            pltpu.HBM((6 * blocks, SEGW), jnp.float32),
            jax.ShapeDtypeStruct((SUB, SEGW), jnp.float32),
        ),
        in_specs=[hbm, hbm, hbm, hbm],
        out_specs=(hbm, vmem),
        scratch_shapes=[
            pltpu.VMEM((6 * groups * span, SEGW), jnp.float32),
            pltpu.VMEM((6 * blocks, SEGW), jnp.float32),
            pltpu.VMEM((1, blocks), jnp.int32),
            pltpu.VMEM((1, blocks), jnp.int32),
            pltpu.SMEM((1, blocks), jnp.int32),
            pltpu.SemaphoreType.DMA((6 * groups,)),
            pltpu.SemaphoreType.DMA((devices // at_once,)),
            pltpu.SemaphoreType.DMA((2,)),
        ],
        compiler_params=pltpu.CompilerParams(vmem_limit_bytes=20 << 20),
        name="pack",
    )(*(in_hbm(x) for x in xs), in_hbm(slots))


def unpack_step(arrived, first_rows, scaled, devices, per_peer, segments):
    groups, _, half_rows, _ = scaled.shape
    span = half_rows + PAD
    blocks = devices * per_peer
    message = 3 * per_peer
    tile = 4 * SUB
    at_once = 8
    part = at_once * 2 * message

    def kernel(in_ref, row_ref, grad_ref, o0, o1, o2, held, came, row_s, sems, in_sems, row_sem):
        to_smem = pltpu.make_async_copy(row_ref, row_s, row_sem)
        to_smem.start()
        coming = []
        for n in range(devices // at_once):
            rows = pl.ds(n * part, part)
            coming.append(pltpu.make_async_copy(in_ref.at[rows], came.at[rows], in_sems.at[n]))
            coming[-1].start()
        to_smem.wait()

        def peer(i, carry):
            for q in range(per_peer):
                row = row_s[0, i * per_peer + q]
                held[pl.ds(row, 6, stride=span), :] = came[
                    pl.ds(i * 2 * message + q, 6, stride=per_peer), :
                ]
            return carry

        for n in range(devices // at_once):
            coming[n].wait()
            lax.fori_loop(n * at_once, (n + 1) * at_once, peer, 0)
        copies = []
        for g in range(groups):
            for k in range(2):
                at = (6 * g + 3 * k) * span

                def update(n, carry, at=at, g=g, k=k):
                    def rows(a):
                        start = pl.multiple_of(at + a * span + n * tile, SUB)
                        return pl.ds(start, tile)

                    scaled_here = grad_ref[g, k, pl.ds(pl.multiple_of(n * tile, SUB), tile), :]
                    old = held[rows(0), :]
                    moment1 = beta_one * held[rows(1), :] + (1.0 - beta_one) * scaled_here
                    moment2 = beta_two * held[rows(2), :] + (1.0 - beta_two) * scaled_here * scaled_here
                    step = moment1 / correct_one / (jnp.sqrt(moment2 / correct_two) + adam_eps)
                    held[rows(0), :] = old - learning_rate * (step + weight_decay * old)
                    held[rows(1), :] = moment1
                    held[rows(2), :] = moment2
                    return carry

                lax.fori_loop(0, half_rows // tile, update, 0)
                for a, o in enumerate((o0, o1, o2)):
                    copies.append(
                        pltpu.make_async_copy(
                            held.at[pl.ds(at + a * span, half_rows)], o.at[g, k], sems.at[6 * g + 3 * k + a]
                        )
                    )
                    copies[-1].start()
        for c in copies:
            c.wait()

    hbm = pl.BlockSpec(memory_space=pltpu.HBM)
    vmem = pl.BlockSpec(memory_space=pltpu.VMEM)
    out = pltpu.HBM(scaled.shape, jnp.float32)
    return pl.pallas_call(
        kernel,
        out_shape=(out, out, out),
        in_specs=[hbm, hbm, vmem],
        out_specs=(hbm, hbm, hbm),
        scratch_shapes=[
            pltpu.VMEM((6 * groups * span, SEGW), jnp.float32),
            pltpu.VMEM((6 * blocks, SEGW), jnp.float32),
            pltpu.SMEM((1, blocks), jnp.int32),
            pltpu.SemaphoreType.DMA((6 * groups,)),
            pltpu.SemaphoreType.DMA((devices // at_once,)),
            pltpu.SemaphoreType.DMA,
        ],
        compiler_params=pltpu.CompilerParams(vmem_limit_bytes=20 << 20),
        name="unpack_step",
    )(in_hbm(arrived), in_hbm(first_rows), scaled)


def sum_over(value, axes):
    for axis in axes:
        count = lax.axis_size(axis)
        apart = 1
        while apart < count:
            route = [(n, n ^ apart) for n in range(count)]
            value = value + lax.ppermute(value, axis, route)
            apart *= 2
    return value


def per_device(total, master_old, moment1_old, moment2_old, grad, send_slots, recv_slots):
    rows, columns = master_old.shape
    segments = columns // 2 // SEGW
    groups, half_rows = rows // SUB, SUB * segments
    devices = lax.axis_size(DP)
    per_peer = rows * segments // devices
    xs = [tiled(x, groups, half_rows) for x in (master_old, moment1_old, moment2_old)]
    packed, mark = pack(xs, send_slots, devices, per_peer, segments)
    outgoing = packed.reshape(2 * devices, 3 * per_peer, 1, SEGW)
    arrived = lax.all_to_all(outgoing, DP_SIDE, split_axis=0, concat_axis=0, tiled=True)
    arrived = arrived.reshape(6 * devices * per_peer, SEGW)

    grad, recv_slots, mark = lax.optimization_barrier((grad, recv_slots, mark))
    first_rows = slot_rows(recv_slots, segments, half_rows + PAD)
    wide = grad.astype(jnp.float32)
    sum_squares = sum_over(jnp.sum(wide * wide).reshape(1, 1), DP_TENSOR)
    limit = clip_ratio * jnp.sqrt(jnp.float32(total))
    clip_scale = jnp.minimum(1.0, limit / jnp.sqrt(sum_squares + 1e-06))
    scaled = tiled(clip_scale * wide, groups, half_rows)
    outs = unpack_step(arrived, first_rows, scaled, devices, per_peer, segments)
    return tuple(untiled(o, rows, columns) for o in outs)


def solution(mesh):
    split = Mesh(mesh.devices.reshape(8, 4, 2, mesh.shape["tensor"] // 2, 2), DP_TENSOR)
    wide_spec = P(DP, ("pair", "side"))

    def whole(master_old, *rest):
        def body(*args):
            return per_device(master_old.size, *args)

        return jax.shard_map(
            body,
            mesh=split,
            in_specs=(wide_spec,) * 4 + (P(DP, None),) * 2,
            out_specs=(wide_spec,) * 3,
            check_vma=False,
        )(master_old, *rest)

    return whole
```

```python
import math

import jax
import jax.numpy as jnp
from jax import lax
from jax.experimental import pallas as pl
from jax.experimental.pallas import tpu as pltpu
from jax.sharding import Mesh
from jax.sharding import PartitionSpec as P

SEGW = 128
SUB = 8
DP = ("dp_0", "dp_1", "dp_2")
DP_TENSOR = ("dp_0", "dp_1", "dp_2", "pair", "side")
DP_SIDE = ("dp_0", "dp_1", "dp_2", "side")
PAD = 8

beta_one = 0.9
beta_two = 0.95
correct_one = 0.6513215599
correct_two = 0.4012630608
adam_eps = 1e-08
learning_rate = 0.01
weight_decay = 0.1
clip_ratio = 0.75


def tiled(x, groups, half_rows):
    rows, columns = x.shape
    tiles = x.reshape(groups, SUB, columns // SEGW, SEGW).transpose(0, 2, 1, 3)
    return tiles.reshape(groups, 2, half_rows, SEGW)


def untiled(x, rows, columns):
    groups = rows // SUB
    tiles = x.reshape(groups, columns // SEGW, SUB, SEGW).transpose(0, 2, 1, 3)
    return tiles.reshape(rows, columns)


def in_hbm(x):
    return pltpu.with_memory_space_constraint(x, pltpu.HBM)


def slot_rows(slots, segments, span):
    r = lax.shift_right_logical(slots * (-(-65536 // segments)), 16)
    s = slots - r * segments
    return lax.shift_right_logical(r, 3) * (6 * span) + s * SUB + (r & (SUB - 1))


def pack(xs, slots, side, devices, per_peer, segments):
    groups, _, half_rows, _ = xs[0].shape
    span = half_rows + PAD
    blocks = devices * per_peer
    message = 3 * per_peer + 1
    both = 2 * message
    at_once = 8
    part = at_once * both

    def kernel(side_ref, x0, x1, x2, slot_ref, out, held, sent, slot_v, row_v, row_s, sems, out_sems, row_sems):
        to_vmem = pltpu.make_async_copy(slot_ref, slot_v, row_sems.at[0])
        to_vmem.start()
        copies = []
        for g in range(groups):
            for k in range(2):
                for a, x in enumerate((x0, x1, x2)):
                    at = 6 * g + 3 * k + a
                    copies.append(
                        pltpu.make_async_copy(
                            x.at[g, k], held.at[pl.ds(at * span, half_rows)], sems.at[at]
                        )
                    )
        for c in copies:
            c.start()
        to_vmem.wait()
        row_v[...] = slot_rows(slot_v[...], segments, span)
        to_smem = pltpu.make_async_copy(row_v, row_s, row_sems.at[1])
        to_smem.start()
        to_smem.wait()
        for c in copies:
            c.wait()

        here = side_ref[0]

        def peer(j, carry):
            start = j * both + 1 - here
            for q in range(per_peer):
                row = row_s[0, j * per_peer + q]
                sent[pl.ds(start + q, 6, stride=per_peer), :] = held[pl.ds(row, 6, stride=span), :]
            return carry

        leaving = []
        for n in range(devices // at_once):
            lax.fori_loop(n * at_once, (n + 1) * at_once, peer, 0)
            last = n * part + both - 2
            moved = sent[pl.ds(last - here * (message - 1), at_once, stride=both), :]
            sent[pl.ds(last, at_once, stride=both), :] = moved
            rows = pl.ds(n * part, part)
            leaving.append(pltpu.make_async_copy(sent.at[rows], out.at[rows], out_sems.at[n]))
            leaving[-1].start()
        for c in leaving:
            c.wait()

    hbm = pl.BlockSpec(memory_space=pltpu.HBM)
    vmem = pl.BlockSpec(memory_space=pltpu.VMEM)
    smem = pl.BlockSpec(memory_space=pltpu.SMEM)
    return pl.pallas_call(
        kernel,
        out_shape=pltpu.HBM((devices * both, SEGW), jnp.float32),
        in_specs=[smem, hbm, hbm, hbm, hbm],
        out_specs=hbm,
        scratch_shapes=[
            pltpu.VMEM((6 * groups * span, SEGW), jnp.float32),
            pltpu.VMEM((devices * both, SEGW), jnp.float32),
            pltpu.VMEM((1, blocks), jnp.int32),
            pltpu.VMEM((1, blocks), jnp.int32),
            pltpu.SMEM((1, blocks), jnp.int32),
            pltpu.SemaphoreType.DMA((6 * groups,)),
            pltpu.SemaphoreType.DMA((devices // at_once,)),
            pltpu.SemaphoreType.DMA((2,)),
        ],
        compiler_params=pltpu.CompilerParams(vmem_limit_bytes=20 << 20),
        name="pack",
    )(side, *(in_hbm(x) for x in xs), in_hbm(slots))


def stamp(packed, side, sums, devices):
    both = packed.shape[0] // devices
    last = both - 1

    def kernel(side_ref, one_ref, two_ref, packed_ref, out, row, sems):
        row[...] = jnp.broadcast_to(one_ref[...] + two_ref[...], row.shape)
        copies = [
            pltpu.make_async_copy(row, out.at[:, side_ref[0] * (both // 2 - 1)], sems.at[0]),
            pltpu.make_async_copy(row, out.at[:, last], sems.at[1]),
        ]
        for c in copies:
            c.start()
        for c in copies:
            c.wait()

    smem = pl.BlockSpec(memory_space=pltpu.SMEM)
    vmem = pl.BlockSpec(memory_space=pltpu.VMEM)
    hbm = pl.BlockSpec(memory_space=pltpu.HBM)
    shape = (devices, both, 1, SEGW)
    return pl.pallas_call(
        kernel,
        out_shape=pltpu.HBM(shape, jnp.float32),
        in_specs=[smem, vmem, vmem, hbm],
        out_specs=hbm,
        input_output_aliases={3: 0},
        scratch_shapes=[pltpu.VMEM((devices, 1, SEGW), jnp.float32), pltpu.SemaphoreType.DMA((2,))],
        compiler_params=pltpu.CompilerParams(vmem_limit_bytes=4 << 20),
        name="stamp",
    )(side, *sums, in_hbm(packed.reshape(shape)))


def unpack_step(arrived, first_rows, wide, side, limit, devices, per_peer, segments):
    groups, _, half_rows, _ = wide.shape
    span = half_rows + PAD
    blocks = devices * per_peer
    message = 3 * per_peer + 1
    both = 2 * message
    tile = 4 * SUB
    at_once = 8
    part = at_once * both

    def kernel(side_ref, in_ref, row_ref, grad_ref, o0, o1, o2, held, came, row_s, sems, in_sems, row_sem):
        to_smem = pltpu.make_async_copy(row_ref, row_s, row_sem)
        to_smem.start()
        coming = []
        for n in range(devices // at_once):
            rows = pl.ds(n * part, part)
            coming.append(pltpu.make_async_copy(in_ref.at[rows], came.at[rows], in_sems.at[n]))
            coming[-1].start()
        to_smem.wait()
        here = side_ref[0]

        def peer(i, carry):
            start = i * both + 1 - here
            for q in range(per_peer):
                row = row_s[0, i * per_peer + q]
                held[pl.ds(row, 6, stride=span), :] = came[pl.ds(start + q, 6, stride=per_peer), :]
            return carry

        sums = jnp.zeros((at_once, SEGW), jnp.float32)
        for n in range(devices // at_once):
            coming[n].wait()
            first = pl.ds(n * part + here * (message - 1), at_once, stride=both)
            sums += came[first, :] + came[pl.ds(n * part + both - 1, at_once, stride=both), :]
            came[first, :] = came[pl.ds(n * part + both - 2, at_once, stride=both), :]
            lax.fori_loop(n * at_once, (n + 1) * at_once, peer, 0)
        sum_squares = jnp.sum(sums, axis=0, keepdims=True)
        clip_scale = jnp.minimum(1.0, limit / jnp.sqrt(sum_squares + 1e-06))
        copies = []
        for g in range(groups):
            for k in range(2):
                at = (6 * g + 3 * k) * span

                def update(n, carry, at=at, g=g, k=k):
                    def rows(a):
                        start = pl.multiple_of(at + a * span + n * tile, SUB)
                        return pl.ds(start, tile)

                    scaled_here = clip_scale * grad_ref[g, k, pl.ds(pl.multiple_of(n * tile, SUB), tile), :]
                    old = held[rows(0), :]
                    moment1 = beta_one * held[rows(1), :] + (1.0 - beta_one) * scaled_here
                    moment2 = beta_two * held[rows(2), :] + (1.0 - beta_two) * scaled_here * scaled_here
                    step = moment1 / correct_one / (jnp.sqrt(moment2 / correct_two) + adam_eps)
                    held[rows(0), :] = old - learning_rate * (step + weight_decay * old)
                    held[rows(1), :] = moment1
                    held[rows(2), :] = moment2
                    return carry

                lax.fori_loop(0, half_rows // tile, update, 0)
                for a, o in enumerate((o0, o1, o2)):
                    copies.append(
                        pltpu.make_async_copy(
                            held.at[pl.ds(at + a * span, half_rows)], o.at[g, k], sems.at[6 * g + 3 * k + a]
                        )
                    )
                    copies[-1].start()
        for c in copies:
            c.wait()

    hbm = pl.BlockSpec(memory_space=pltpu.HBM)
    vmem = pl.BlockSpec(memory_space=pltpu.VMEM)
    smem = pl.BlockSpec(memory_space=pltpu.SMEM)
    out = pltpu.HBM(wide.shape, jnp.float32)
    return pl.pallas_call(
        kernel,
        out_shape=(out, out, out),
        in_specs=[smem, hbm, hbm, vmem],
        out_specs=(hbm, hbm, hbm),
        scratch_shapes=[
            pltpu.VMEM((6 * groups * span, SEGW), jnp.float32),
            pltpu.VMEM((devices * both, SEGW), jnp.float32),
            pltpu.SMEM((1, blocks), jnp.int32),
            pltpu.SemaphoreType.DMA((6 * groups,)),
            pltpu.SemaphoreType.DMA((devices // at_once,)),
            pltpu.SemaphoreType.DMA,
        ],
        compiler_params=pltpu.CompilerParams(vmem_limit_bytes=20 << 20),
        name="unpack_step",
    )(side, in_hbm(arrived), in_hbm(first_rows), wide)


def per_device(total, master_old, moment1_old, moment2_old, grad, send_slots, recv_slots):
    rows, columns = master_old.shape
    segments = columns // 2 // SEGW
    groups, half_rows = rows // SUB, SUB * segments
    devices = lax.axis_size(DP)
    per_peer = rows * segments // devices
    xs = [tiled(x, groups, half_rows) for x in (master_old, moment1_old, moment2_old)]
    side = lax.axis_index("side").astype(jnp.int32).reshape(1)

    wide = grad.astype(jnp.float32)
    own_sum = jnp.sum(wide * wide).reshape(1, 1)
    other_sum = lax.ppermute(own_sum, "pair", [(0, 1), (1, 0)])
    packed = pack(xs, send_slots, side, devices, per_peer, segments)
    outgoing = stamp(packed, side, (own_sum, other_sum), devices)
    outgoing = outgoing.reshape(2 * devices, 3 * per_peer + 1, 1, SEGW)
    arrived = lax.all_to_all(outgoing, DP_SIDE, split_axis=0, concat_axis=0, tiled=True)
    arrived = arrived.reshape(packed.shape)

    first_rows = slot_rows(recv_slots, segments, half_rows + PAD)
    limit = clip_ratio * math.sqrt(total)
    outs = unpack_step(
        arrived, first_rows, tiled(wide, groups, half_rows), side, limit, devices, per_peer, segments
    )
    return tuple(untiled(o, rows, columns) for o in outs)


def solution(mesh):
    split = Mesh(mesh.devices.reshape(8, 4, 2, mesh.shape["tensor"] // 2, 2), DP_TENSOR)
    wide_spec = P(DP, ("pair", "side"))

    def whole(master_old, *rest):
        def body(*args):
            return per_device(master_old.size, *args)

        return jax.shard_map(
            body,
            mesh=split,
            in_specs=(wide_spec,) * 4 + (P(DP, None),) * 2,
            out_specs=(wide_spec,) * 3,
            check_vma=False,
        )(master_old, *rest)

    return whole
```

```python
import math

import jax
import jax.numpy as jnp
from jax import lax
from jax.experimental import pallas as pl
from jax.experimental.pallas import tpu as pltpu
from jax.sharding import Mesh
from jax.sharding import PartitionSpec as P

SEGW = 128
SUB = 8
DP = ("dp_0", "dp_1", "dp_2")
DP_TENSOR = ("dp_0", "dp_1", "dp_2", "pair", "side")
DP_SIDE = ("dp_0", "dp_1", "dp_2", "side")
PAD = 8

beta_one = 0.9
beta_two = 0.95
correct_one = 0.6513215599
correct_two = 0.4012630608
adam_eps = 1e-08
learning_rate = 0.01
weight_decay = 0.1
clip_ratio = 0.75


def tiled(x, groups, half_rows):
    rows, columns = x.shape
    tiles = x.reshape(groups, SUB, columns // SEGW, SEGW).transpose(0, 2, 1, 3)
    return tiles.reshape(groups, 2, half_rows, SEGW)


def untiled(x, rows, columns):
    groups = rows // SUB
    tiles = x.reshape(groups, columns // SEGW, SUB, SEGW).transpose(0, 2, 1, 3)
    return tiles.reshape(rows, columns)


def in_vmem(x):
    return pltpu.with_memory_space_constraint(x, pltpu.VMEM)


def in_hbm(x):
    return pltpu.with_memory_space_constraint(x, pltpu.HBM)


def slot_rows(slots, segments, span):
    r = lax.shift_right_logical(slots * (-(-65536 // segments)), 16)
    s = slots - r * segments
    return lax.shift_right_logical(r, 3) * (6 * span) + s * SUB + (r & (SUB - 1))


def pack(xs, slots, new_slots, side, devices, per_peer, segments):
    groups, _, half_rows, _ = xs[0].shape
    span = half_rows + PAD
    blocks = devices * per_peer
    message = 3 * per_peer + 1
    both = 2 * message

    def kernel(side_ref, x0, x1, x2, slot_ref, new_ref, sent, new_rows, held, slot_v, new_v, row_v, row_s, sems, row_sems):
        to_vmem = pltpu.make_async_copy(slot_ref, slot_v, row_sems.at[0])
        to_vmem.start()
        new_to_vmem = pltpu.make_async_copy(new_ref, new_v, row_sems.at[2])
        new_to_vmem.start()
        copies = []
        for g in range(groups):
            for k in range(2):
                for a, x in enumerate((x0, x1, x2)):
                    at = 6 * g + 3 * k + a
                    copies.append(
                        pltpu.make_async_copy(
                            x.at[g, k], held.at[pl.ds(at * span, half_rows)], sems.at[at]
                        )
                    )
        for c in copies:
            c.start()
        to_vmem.wait()
        row_v[...] = slot_rows(slot_v[...], segments, span)
        to_smem = pltpu.make_async_copy(row_v, row_s, row_sems.at[1])
        to_smem.start()
        new_to_vmem.wait()
        new_rows[...] = slot_rows(new_v[...], segments, span)
        to_smem.wait()
        for c in copies:
            c.wait()

        here = side_ref[0]

        def peer(j, carry):
            start = j * both + 1 - here
            for q in range(per_peer):
                row = row_s[0, j * per_peer + q]
                sent[pl.ds(start + q, 6, stride=per_peer), :] = held[pl.ds(row, 6, stride=span), :]
            return carry

        lax.fori_loop(0, devices, peer, 0)
        for n in range(devices // SUB):
            last = n * SUB * both + both - 2
            moved = sent[pl.ds(last - here * (message - 1), SUB, stride=both), :]
            sent[pl.ds(last, SUB, stride=both), :] = moved

    hbm = pl.BlockSpec(memory_space=pltpu.HBM)
    vmem = pl.BlockSpec(memory_space=pltpu.VMEM)
    smem = pl.BlockSpec(memory_space=pltpu.SMEM)
    return pl.pallas_call(
        kernel,
        out_shape=(
            pltpu.VMEM((devices * both, SEGW), jnp.float32),
            jax.ShapeDtypeStruct((1, blocks), jnp.int32),
        ),
        in_specs=[smem, hbm, hbm, hbm, hbm, hbm],
        out_specs=(vmem, vmem),
        scratch_shapes=[
            pltpu.VMEM((6 * groups * span, SEGW), jnp.float32),
            pltpu.VMEM((1, blocks), jnp.int32),
            pltpu.VMEM((1, blocks), jnp.int32),
            pltpu.VMEM((1, blocks), jnp.int32),
            pltpu.SMEM((1, blocks), jnp.int32),
            pltpu.SemaphoreType.DMA((6 * groups,)),
            pltpu.SemaphoreType.DMA((3,)),
        ],
        compiler_params=pltpu.CompilerParams(vmem_limit_bytes=20 << 20),
        name="pack",
    )(side, *(in_hbm(x) for x in xs), in_hbm(slots), in_hbm(new_slots))


def stamp(packed, side, sums, devices):
    both = packed.shape[0] // devices

    def kernel(side_ref, one_ref, two_ref, packed_ref, out):
        row = jnp.broadcast_to(one_ref[...] + two_ref[...], (SUB, SEGW))
        for n in range(devices // SUB):
            start = n * SUB * both
            out[pl.ds(start + side_ref[0] * (both // 2 - 1), SUB, stride=both), :] = row
            out[pl.ds(start + both - 1, SUB, stride=both), :] = row

    smem = pl.BlockSpec(memory_space=pltpu.SMEM)
    vmem = pl.BlockSpec(memory_space=pltpu.VMEM)
    return pl.pallas_call(
        kernel,
        out_shape=pltpu.VMEM(packed.shape, jnp.float32),
        in_specs=[smem, vmem, vmem, vmem],
        out_specs=vmem,
        input_output_aliases={3: 0},
        compiler_params=pltpu.CompilerParams(vmem_limit_bytes=16 << 20),
        name="stamp",
    )(side, *sums, in_vmem(packed))


def unpack_step(arrived, first_rows, grad, side, limit, devices, per_peer, segments):
    groups, _, half_rows, _ = grad.shape
    span = half_rows + PAD
    blocks = devices * per_peer
    message = 3 * per_peer + 1
    both = 2 * message
    tile = 4 * SUB

    def kernel(side_ref, came, row_ref, grad_ref, o0, o1, o2, held, row_s, sems, row_sem):
        to_smem = pltpu.make_async_copy(row_ref, row_s, row_sem)
        to_smem.start()
        here = side_ref[0]
        sums = jnp.zeros((SUB, SEGW), jnp.float32)
        for n in range(devices // SUB):
            first = n * SUB * both
            sums += came[pl.ds(first + here * (message - 1), SUB, stride=both), :]
            sums += came[pl.ds(first + both - 1, SUB, stride=both), :]
        sum_squares = jnp.sum(sums, axis=0, keepdims=True)
        clip_scale = jnp.minimum(1.0, limit / jnp.sqrt(sum_squares + 1e-06))
        to_smem.wait()

        def peer(i, carry):
            start = i * both + 1 - here
            for q in range(per_peer):
                row = row_s[0, i * per_peer + q]
                held[pl.ds(row, 6, stride=span), :] = came[pl.ds(start + q, 6, stride=per_peer), :]
            row = row_s[0, i * per_peer] + 3 * span
            held[pl.ds(row, 1), :] = came[pl.ds(i * both + message + here * (message - 2), 1), :]
            return carry

        lax.fori_loop(0, devices, peer, 0)
        copies = []
        for g in range(groups):
            for k in range(2):
                at = (6 * g + 3 * k) * span

                def update(n, carry, at=at, g=g, k=k):
                    def rows(a):
                        start = pl.multiple_of(at + a * span + n * tile, SUB)
                        return pl.ds(start, tile)

                    scaled_here = clip_scale * grad_ref[
                        g, k, pl.ds(pl.multiple_of(n * tile, SUB), tile), :
                    ].astype(jnp.float32)
                    old = held[rows(0), :]
                    moment1 = beta_one * held[rows(1), :] + (1.0 - beta_one) * scaled_here
                    moment2 = beta_two * held[rows(2), :] + (1.0 - beta_two) * scaled_here * scaled_here
                    step = moment1 / correct_one / (jnp.sqrt(moment2 / correct_two) + adam_eps)
                    held[rows(0), :] = old - learning_rate * (step + weight_decay * old)
                    held[rows(1), :] = moment1
                    held[rows(2), :] = moment2
                    return carry

                lax.fori_loop(0, half_rows // tile, update, 0)
                for a, o in enumerate((o0, o1, o2)):
                    copies.append(
                        pltpu.make_async_copy(
                            held.at[pl.ds(at + a * span, half_rows)], o.at[g, k], sems.at[6 * g + 3 * k + a]
                        )
                    )
                    copies[-1].start()
        for c in copies:
            c.wait()

    hbm = pl.BlockSpec(memory_space=pltpu.HBM)
    vmem = pl.BlockSpec(memory_space=pltpu.VMEM)
    smem = pl.BlockSpec(memory_space=pltpu.SMEM)
    out = pltpu.HBM(grad.shape, jnp.float32)
    return pl.pallas_call(
        kernel,
        out_shape=(out, out, out),
        in_specs=[smem, vmem, hbm, vmem],
        out_specs=(hbm, hbm, hbm),
        scratch_shapes=[
            pltpu.VMEM((6 * groups * span, SEGW), jnp.float32),
            pltpu.SMEM((1, blocks), jnp.int32),
            pltpu.SemaphoreType.DMA((6 * groups,)),
            pltpu.SemaphoreType.DMA,
        ],
        compiler_params=pltpu.CompilerParams(vmem_limit_bytes=20 << 20),
        name="unpack_step",
    )(side, in_vmem(arrived), in_hbm(first_rows), grad)


def per_device(total, master_old, moment1_old, moment2_old, grad, send_slots, recv_slots):
    rows, columns = master_old.shape
    segments = columns // 2 // SEGW
    groups, half_rows = rows // SUB, SUB * segments
    devices = lax.axis_size(DP)
    per_peer = rows * segments // devices
    xs = [tiled(x, groups, half_rows) for x in (master_old, moment1_old, moment2_old)]
    side = lax.axis_index("side").astype(jnp.int32).reshape(1)

    wide = grad.astype(jnp.float32)
    own_sum = jnp.sum(wide * wide).reshape(1, 1)
    other_sum = lax.ppermute(own_sum, "pair", [(0, 1), (1, 0)])
    packed, first_rows = pack(xs, send_slots, recv_slots, side, devices, per_peer, segments)
    outgoing = stamp(packed, side, (own_sum, other_sum), devices)
    outgoing = outgoing.reshape(2 * devices, 3 * per_peer + 1, 1, SEGW)
    arrived = lax.all_to_all(outgoing, DP_SIDE, split_axis=0, concat_axis=0, tiled=True)
    arrived = arrived.reshape(packed.shape)

    limit = clip_ratio * math.sqrt(total)
    outs = unpack_step(
        arrived, first_rows, tiled(grad, groups, half_rows), side, limit, devices, per_peer, segments
    )
    return tuple(untiled(o, rows, columns) for o in outs)


def solution(mesh):
    split = Mesh(mesh.devices.reshape(8, 4, 2, mesh.shape["tensor"] // 2, 2), DP_TENSOR)
    wide_spec = P(DP, ("pair", "side"))

    def whole(master_old, *rest):
        def body(*args):
            return per_device(master_old.size, *args)

        return jax.shard_map(
            body,
            mesh=split,
            in_specs=(wide_spec,) * 4 + (P(DP, None),) * 2,
            out_specs=(wide_spec,) * 3,
            check_vma=False,
        )(master_old, *rest)

    return whole
```
